32 devices in a mesh: dp: 2 (over y), fsdp: 4 (over z), tensor: 4 (over x, core).
Axes of the slice: x: 2, y: 2, z: 4, core: 2. Of those that a mesh axis runs over, the one named last changes fastest.
Arguments:
- tokens: bfloat16 [2048, 8192], P(('dp', 'fsdp')), may hold values from -40 to 40
- next_tokens: bfloat16 [2048, 8192], P(('dp', 'fsdp')), may hold values from -6 to 6
- cotangent: bfloat16 [2, 2048, 1024], P(None, ('dp', 'fsdp'), 'tensor'), may hold values from -6 to 6
- master: float32 [2, 8192, 1024], P(None, 'fsdp', 'tensor'), may hold values from -0.0625 to 0.0625
- first_moment: float32 [2, 8192, 1024], P(None, 'fsdp', 'tensor'), may hold values from -6 to 6
- second_moment: float32 [2, 8192, 1024], P(None, 'fsdp', 'tensor'), may hold values from 0.25 to 4
Outputs:
- new_master: float32 [2, 8192, 1024], P(None, 'fsdp', 'tensor')
- new_first: float32 [2, 8192, 1024], P(None, 'fsdp', 'tensor')
- new_second: float32 [2, 8192, 1024], P(None, 'fsdp', 'tensor')
- projected: bfloat16 [2, 2048, 1024], P(None, ('dp', 'fsdp'), 'tensor')
The draws below stay inside these ranges and needn't reach their ends.
All inputs are finite; a program needn't handle non-finite values.
Results may differ from the reference program's by a relative error of at most 0.005.
Values may be sent and summed in bfloat16 or wider, within the bound.
No kernel may reach another device: no remote copies, remote signals or barrier semaphores. Data moves between devices by JAX's collectives and lax.ppermute only.
A program may use at most 128 MiB of HBM per device.

```python
import math
import jax
import jax.numpy as jnp

D = 8192
KVW = 1024
STEP = 10
TOKENS = 2048
N_FSDP = 4


def draw_tokens(key, part):
    key_values = jax.random.fold_in(key, 11)
    key_rough = jax.random.fold_in(key, 12)
    column = jnp.arange(D).astype(jnp.float32)
    block = D // N_FSDP
    outer = column / D
    inner = (jnp.arange(D) % block).astype(jnp.float32) / block
    rough = jax.random.uniform(key_rough, (D,), jnp.float32, 0.6, 1.4)
    rise = jnp.exp(jnp.log(4.0) * outer + jnp.log(3.0) * inner)
    values = jnp.clip(jax.random.normal(key_values, (TOKENS, D), jnp.float32), -4.0, 4.0)
    result = values * (rise * rough)[None, :]
    return jnp.clip(result, -40.0, 40.0).astype(jnp.bfloat16)


def block_scale(stream_key, dims, pieces, least, largest):
    loudness = 1.0
    for axis_at, parts in pieces:
        steps = jax.random.uniform(jax.random.fold_in(jax.random.fold_in(stream_key, 6), axis_at), (parts,), jnp.float32, least / len(pieces), largest / len(pieces))
        loudness = loudness * jnp.repeat(jnp.exp(steps), dims[axis_at] // parts).reshape((-1,) + (1,) * (len(dims) - 1 - axis_at))
    return loudness


def normal_values(rng, shape, width, reach, shards=(), held_as=jnp.bfloat16):
    drawn = width * jax.random.normal(rng, shape, jnp.float32)
    if shards:
        drawn = drawn * block_scale(rng, shape, shards, -0.22, 0.18)
    return jnp.clip(drawn, -reach, reach).astype(held_as)


def setup_inputs(seed: int = 0) -> dict:
    arg_keys = jax.random.split(jax.random.key(seed), 7)
    return {
        "tokens": draw_tokens(jax.random.fold_in(arg_keys[6], 71), 0),
        "next_tokens": normal_values(arg_keys[1], (TOKENS, D), 1.0, 6.0, ((0, 8),)),
        "cotangent": normal_values(arg_keys[2], (2, TOKENS, KVW), 1.0, 6.0, ((1, 8), (2, 4))),
        "master": normal_values(arg_keys[3], (2, D, KVW), D ** -0.5, 0.0625, ((1, 4), (2, 4)), jnp.float32),
        "first_moment": normal_values(arg_keys[4], (2, D, KVW), 1.0, 6.0, ((1, 4), (2, 4)), jnp.float32),
        "second_moment": jnp.clip(jnp.exp(math.log(4.0) - 2.7725887 * jax.random.uniform(arg_keys[5], (2, D, KVW), jnp.float32) ** block_scale(arg_keys[5], (2, D, KVW), ((1, 4), (2, 4)), -0.2, 0.2)), 0.25, 4.0),
    }


def reference(tokens, next_tokens, cotangent, master, first_moment, second_moment):
    grad = jnp.stack([jnp.dot(tokens.T, cotangent[s], preferred_element_type=jnp.float32) for s in range(2)])
    total = jnp.sum(grad * grad)
    scale = jnp.minimum(1.0, 1.0 / jnp.sqrt(total / (2 * D * KVW) + 1e-06))
    clipped = scale * grad
    new_first = 0.9 * first_moment + 0.1 * clipped
    new_second = 0.95 * second_moment + 0.05 * clipped * clipped
    first_hat = new_first / (1.0 - 0.9 ** STEP)
    second_hat = new_second / (1.0 - 0.95 ** STEP)
    new_master = master - 0.003 * (first_hat / (jnp.sqrt(second_hat) + 1e-08) + 0.1 * master)
    weight = new_master.astype(jnp.bfloat16)
    projected = jnp.stack([jnp.dot(next_tokens, weight[s], preferred_element_type=jnp.float32) for s in range(2)])
    return (new_master, new_first, new_second, projected.astype(jnp.bfloat16))
```

```python
import functools

import jax
import jax.numpy as jnp
from jax import lax
from jax.experimental import pallas as pl
from jax.experimental.pallas import tpu as pltpu
from jax.sharding import PartitionSpec as P

STEP = 10
VMEM = pl.BlockSpec(memory_space=pltpu.VMEM)
SMEM = pl.BlockSpec(memory_space=pltpu.SMEM)


def shift(x, axis, k):
    n = lax.axis_size(axis)
    return lax.ppermute(x, axis, [(i, (i + k) % n) for i in range(n)])


def swap(x, axis, stride):
    n = lax.axis_size(axis)
    return lax.ppermute(x, axis, [(i, i ^ stride) for i in range(n)])


def spread(x, axis):
    pieces = {0: x}
    stride = lax.axis_size(axis) // 2
    while stride:
        pieces |= {r ^ stride: swap(piece, axis, stride) for r, piece in pieces.items()}
        stride //= 2
    return [pieces[r] for r in range(lax.axis_size(axis))]


def contract_rows(a, b):
    return lax.dot_general(a, b, (((0,), (0,)), ((), ())), preferred_element_type=jnp.float32)


def grad_kernel(n_f, n_t, own, at_ref, *refs):
    first, rest, cots, refs = refs[:n_t], refs[n_t : 2 * n_t], refs[2 * n_t : 2 * n_t + n_f], refs[2 * n_t + n_f :]
    rows = cots[0].shape[1]
    chunk = rest[0].shape[1]
    squares = jnp.zeros((8, 128), jnp.float32)
    for r in range(n_t):
        at = pl.multiple_of((at_ref[0] ^ r) * chunk, chunk)
        for s in range(2):
            acc = contract_rows(first[r][...], cots[0][s])
            for k in range(1, n_f):
                acc += contract_rows(rest[r][(k - 1) * rows : k * rows, :], cots[k][s])
            if own:
                refs[0][s, pl.ds(at, chunk), :] = acc
            else:
                acc += refs[0][s, pl.ds(at, chunk), :]
                refs[1][s, pl.ds(at, chunk), :] = acc
                squares += jnp.sum((acc * acc).reshape(-1, 8, 128), axis=0)
    if not own:
        refs[2][...] = squares


def clip_scale(squares, count):
    total = jnp.sum(squares)
    return jnp.minimum(1.0, 1.0 / jnp.sqrt(jnp.full((8, 128), total / count, jnp.float32) + 1e-06))[:1, :1]


def adam_update(scale, grad, master, first_moment, second_moment):
    clipped = scale * grad
    new_first = 0.9 * first_moment + 0.1 * clipped
    new_second = 0.95 * second_moment + 0.05 * clipped * clipped
    first_hat = new_first / (1.0 - 0.9**STEP)
    second_hat = new_second / (1.0 - 0.95**STEP)
    new_master = master - 0.003 * (first_hat / (jnp.sqrt(second_hat) + 1e-08) + 0.1 * master)
    return (new_master, new_first, new_second)


def project_kernel(n_f, n_t, count, at_ref, squares_ref, grad_ref, master_ref, m_ref, v_ref, own_ref, *refs):
    rest, outs, weight = refs[:n_t], refs[n_t:-1], refs[-1]
    rows, chunk = own_ref.shape[0], rest[0].shape[1]
    s, b = pl.program_id(0), pl.program_id(1)
    scale = clip_scale(squares_ref[...], count)
    new_master, _, _ = adam_update(scale, grad_ref[0], master_ref[0], m_ref[0], v_ref[0])
    block = new_master.shape[0]
    weight[s, pl.ds(pl.multiple_of(b * block, block), block), :] = new_master.astype(jnp.bfloat16)

    @pl.when((s == 1) & (b == pl.num_programs(1) - 1))
    def _():
        for s in range(2):
            outs[0][s] = jnp.dot(own_ref[...], weight[s], preferred_element_type=jnp.float32)
            for k in range(1, n_f):
                acc = jnp.zeros(outs[0].shape[1:], jnp.float32)
                for r in range(n_t):
                    at = pl.multiple_of((at_ref[0] ^ r) * chunk, chunk)
                    acc += jnp.dot(
                        rest[r][(k - 1) * rows : k * rows, :],
                        weight[s, pl.ds(at, chunk), :],
                        preferred_element_type=jnp.float32,
                    )
                outs[k][s] = acc.astype(jnp.bfloat16)


def update_kernel(count, squares_ref, grad_ref, master_ref, m_ref, v_ref, new_master_ref, new_m_ref, new_v_ref):
    scale = clip_scale(squares_ref[...], count)
    new_master_ref[...], new_m_ref[...], new_v_ref[...] = adam_update(
        scale.reshape(1, 1, 1), grad_ref[...], master_ref[...], m_ref[...], v_ref[...]
    )


def per_device(tokens, next_tokens, cotangent, master, first_moment, second_moment):
    n_f, n_t = lax.axis_size("fsdp"), lax.axis_size("tensor")
    f, t = lax.axis_index("fsdp"), lax.axis_index("tensor")
    rows, width = tokens.shape
    shard = width // n_f
    chunk = shard // n_t
    kv = cotangent.shape[2]
    count = 2.0 * width * kv * n_t
    at = t.reshape(1).astype(jnp.int32)

    def mine(x, owner, r=0):
        return lax.dynamic_slice(x, (0, owner * shard + (t ^ r) * chunk), (rows, chunk))

    def fetch(x):
        got = [shift(mine(x, (f + k) % n_f), "fsdp", k) for k in range(1, n_f)]
        return jnp.concatenate(got, axis=0)

    first = [mine(tokens, f, r) for r in range(n_t)]
    other_first = spread(shift(first[0], "dp", 1), "tensor")
    rest = fetch(tokens)
    other_rest = spread(shift(rest, "dp", 1), "tensor")
    rest = spread(rest, "tensor")
    cots = [cotangent] + [shift(cotangent, "fsdp", k) for k in range(1, n_f)]
    other_cots = [shift(c, "dp", 1) for c in cots]
    next_block = lax.dynamic_slice(next_tokens, (0, f * shard), (rows, shard))
    next_rest = spread(fetch(next_tokens), "tensor")

    shard_type = jax.ShapeDtypeStruct((2, shard, kv), jnp.float32)
    grad = pl.pallas_call(
        functools.partial(grad_kernel, n_f, n_t, True),
        out_shape=shard_type,
        in_specs=[SMEM] + [VMEM] * (2 * n_t + n_f),
        out_specs=VMEM,
        name="grad_own",
    )(at, *first, *rest, *cots)
    grad, squares = pl.pallas_call(
        functools.partial(grad_kernel, n_f, n_t, False),
        out_shape=(shard_type, jax.ShapeDtypeStruct((8, 128), jnp.float32)),
        in_specs=[SMEM] + [VMEM] * (2 * n_t + n_f + 1),
        out_specs=(VMEM, VMEM),
        name="grad_all",
    )(at, *other_first, *other_rest, *other_cots, grad)

    for axis, n in (("fsdp", n_f), ("tensor", n_t)):
        squares = functools.reduce(jnp.add, [shift(squares, axis, k) for k in range(1, n)], squares)

    block = min(shard, 512)
    tile = pl.BlockSpec((1, block, kv), lambda s, b: (s, b, 0))
    whole = pl.BlockSpec(memory_space=pltpu.VMEM)
    out = (2, rows, kv)
    partial = pl.pallas_call(
        functools.partial(project_kernel, n_f, n_t, count),
        grid=(2, shard // block),
        out_shape=(jax.ShapeDtypeStruct(out, jnp.float32),) + (jax.ShapeDtypeStruct(out, jnp.bfloat16),) * (n_f - 1),
        in_specs=[SMEM, whole] + [tile] * 4 + [whole] * (1 + n_t),
        out_specs=(whole,) * n_f,
        scratch_shapes=[pltpu.VMEM((2, shard, kv), jnp.bfloat16)],
        name="project",
    )(at, squares, grad, master, first_moment, second_moment, next_block, *next_rest)
    got = [shift(partial[k], "fsdp", -k) for k in range(1, n_f)]
    projected = functools.reduce(jnp.add, [g.astype(jnp.float32) for g in got], partial[0])
    new_master, new_first, new_second = pl.pallas_call(
        functools.partial(update_kernel, count),
        grid=(2, shard // block),
        out_shape=(shard_type,) * 3,
        in_specs=[whole] + [tile] * 4,
        out_specs=(tile,) * 3,
        name="update",
    )(squares, grad, master, first_moment, second_moment)
    return (new_master, new_first, new_second, projected.astype(jnp.bfloat16))


def solution(mesh):
    in_specs = (
        P(("dp", "fsdp"), None),
        P(("dp", "fsdp"), None),
        P(None, ("dp", "fsdp"), "tensor"),
        P(None, "fsdp", "tensor"),
        P(None, "fsdp", "tensor"),
        P(None, "fsdp", "tensor"),
    )
    out_specs = (
        P(None, "fsdp", "tensor"),
        P(None, "fsdp", "tensor"),
        P(None, "fsdp", "tensor"),
        P(None, ("dp", "fsdp"), "tensor"),
    )
    return jax.shard_map(
        per_device, mesh=mesh, in_specs=in_specs, out_specs=out_specs, check_vma=False
    )
```

```python
import functools

import jax
import jax.numpy as jnp
from jax import lax
from jax.experimental import pallas as pl
from jax.experimental.pallas import tpu as pltpu
from jax.sharding import PartitionSpec as P

STEP = 10
VMEM = pl.BlockSpec(memory_space=pltpu.VMEM)
SMEM = pl.BlockSpec(memory_space=pltpu.SMEM)


def shift(x, axis, k):
    n = lax.axis_size(axis)
    return lax.ppermute(x, axis, [(i, (i + k) % n) for i in range(n)])


def spread(x, axis):
    n = lax.axis_size(axis)
    pieces = {0: x}
    stride = n // 2
    while stride:
        for r, piece in list(pieces.items()):
            pieces[r ^ stride] = lax.ppermute(piece, axis, [(i, i ^ stride) for i in range(n)])
        stride //= 2
    return [pieces[r] for r in range(n)]


def contract_rows(a, b):
    return lax.dot_general(a, b, (((0,), (0,)), ((), ())), preferred_element_type=jnp.float32)


def row_blocks(refs, rows):
    return [ref[i : i + rows, :] for ref in refs for i in range(0, ref.shape[0], rows)]


def grad_kernel(n_f, n_t, own, groups, at_ref, *refs):
    tokens, cots, refs = refs[: groups * n_t], refs[groups * n_t : groups * n_t + n_f], refs[groups * n_t + n_f :]
    rows, chunk = cots[0].shape[1], tokens[0].shape[1]
    squares = jnp.zeros((8, 128), jnp.float32)
    for r in range(n_t):
        at = pl.multiple_of((at_ref[0] ^ r) * chunk, chunk)
        for s in range(2):
            blocks = row_blocks(tokens[r::n_t], rows)
            acc = functools.reduce(jnp.add, [contract_rows(b, c[s]) for b, c in zip(blocks, cots, strict=True)])
            if own:
                refs[0][s, pl.ds(at, chunk), :] = acc
            else:
                acc += refs[0][s, pl.ds(at, chunk), :]
                refs[1][s, pl.ds(at, chunk), :] = acc
                squares += jnp.sum((acc * acc).reshape(-1, 8, 128), axis=0)
    if not own:
        refs[2][...] = squares


def clip_scale(squares, count):
    total = jnp.sum(squares)
    return jnp.minimum(1.0, 1.0 / jnp.sqrt(jnp.full((8, 128), total / count, jnp.float32) + 1e-06))[:1, :1]


def adam_update(scale, grad, master, first_moment, second_moment):
    clipped = scale * grad
    new_first = 0.9 * first_moment + 0.1 * clipped
    new_second = 0.95 * second_moment + 0.05 * clipped * clipped
    first_hat = new_first / (1.0 - 0.9**STEP)
    second_hat = new_second / (1.0 - 0.95**STEP)
    new_master = master - 0.003 * (first_hat / (jnp.sqrt(second_hat) + 1e-08) + 0.1 * master)
    return (new_master, new_first, new_second)


def project_kernel(n_f, n_t, groups, count, at_ref, squares_ref, grad_ref, master_ref, m_ref, v_ref, own_ref, *refs):
    rest, outs, weight = refs[: groups * n_t], refs[groups * n_t : -1], refs[-1]
    rows, chunk = own_ref.shape[0], rest[0].shape[1]
    s, b = pl.program_id(0), pl.program_id(1)
    scale = clip_scale(squares_ref[...], count)
    new_master, _, _ = adam_update(scale, grad_ref[0], master_ref[0], m_ref[0], v_ref[0])
    block = new_master.shape[0]
    weight[s, pl.ds(pl.multiple_of(b * block, block), block), :] = new_master.astype(jnp.bfloat16)

    @pl.when((s == 1) & (b == pl.num_programs(1) - 1))
    def _():
        for s in range(2):
            outs[0][s] = jnp.dot(own_ref[...], weight[s], preferred_element_type=jnp.float32)
            blocks = [row_blocks(rest[r::n_t], rows) for r in range(n_t)]
            for k in range(1, n_f):
                acc = jnp.zeros(outs[0].shape[1:], jnp.float32)
                for r in range(n_t):
                    at = pl.multiple_of((at_ref[0] ^ r) * chunk, chunk)
                    acc += jnp.dot(
                        blocks[r][k - 1], weight[s, pl.ds(at, chunk), :], preferred_element_type=jnp.float32
                    )
                outs[k][s] = acc.astype(jnp.bfloat16)


def update_kernel(count, squares_ref, grad_ref, master_ref, m_ref, v_ref, new_master_ref, new_m_ref, new_v_ref):
    scale = clip_scale(squares_ref[...], count)
    new_master_ref[...], new_m_ref[...], new_v_ref[...] = adam_update(
        scale.reshape(1, 1, 1), grad_ref[...], master_ref[...], m_ref[...], v_ref[...]
    )


def per_device(tokens, next_tokens, cotangent, master, first_moment, second_moment):
    n_f, n_t = lax.axis_size("fsdp"), lax.axis_size("tensor")
    f, t = lax.axis_index("fsdp"), lax.axis_index("tensor")
    rows, width = tokens.shape
    shard = width // n_f
    chunk = shard // n_t
    kv = cotangent.shape[2]
    count = 2.0 * width * kv * n_t
    at = t.reshape(1).astype(jnp.int32)

    def mine(x, owner, r=0):
        return lax.dynamic_slice(x, (0, owner * shard + (t ^ r) * chunk), (rows, chunk))

    def fetch(x):
        return [shift(mine(x, (f + k) % n_f), "fsdp", k) for k in range(1, n_f)]

    def flat(groups):
        return [piece for group in groups for piece in group]

    first = [mine(tokens, f, r) for r in range(n_t)]
    rest = jnp.concatenate(fetch(tokens), axis=0)
    other_first = spread(shift(first[0], "dp", 1), "tensor")
    other_rest = spread(shift(rest, "dp", 1), "tensor")
    rest = spread(rest, "tensor")
    cots = [cotangent] + [shift(cotangent, "fsdp", k) for k in range(1, n_f)]
    other_cots = [shift(c, "dp", 1) for c in cots]
    next_block = lax.dynamic_slice(next_tokens, (0, f * shard), (rows, shard))
    next_rest = [spread(x, "tensor") for x in fetch(next_tokens)]

    shard_type = jax.ShapeDtypeStruct((2, shard, kv), jnp.float32)
    grad = pl.pallas_call(
        functools.partial(grad_kernel, n_f, n_t, True, 2),
        out_shape=shard_type,
        in_specs=[SMEM] + [VMEM] * (2 * n_t + n_f),
        out_specs=VMEM,
    )(at, *first, *rest, *cots)
    grad, squares = pl.pallas_call(
        functools.partial(grad_kernel, n_f, n_t, False, 2),
        out_shape=(shard_type, jax.ShapeDtypeStruct((8, 128), jnp.float32)),
        in_specs=[SMEM] + [VMEM] * (2 * n_t + n_f + 1),
        out_specs=(VMEM, VMEM),
    )(at, *other_first, *other_rest, *other_cots, grad)

    for axis, n in (("fsdp", n_f), ("tensor", n_t)):
        squares = functools.reduce(jnp.add, [shift(squares, axis, k) for k in range(1, n)], squares)

    block = min(shard, 512)
    tile = pl.BlockSpec((1, block, kv), lambda s, b: (s, b, 0))
    whole = pl.BlockSpec(memory_space=pltpu.VMEM)
    out = (2, rows, kv)
    partial = pl.pallas_call(
      functools.partial(project_kernel, n_f, n_t, n_f - 1, count),
      grid=(2, shard // block),
      out_shape=(jax.ShapeDtypeStruct(out, jnp.float32),) + (jax.ShapeDtypeStruct(out, jnp.bfloat16),) * (n_f - 1),
      in_specs=[SMEM, whole] + [tile] * 4 + [whole] * (1 + (n_f - 1) * n_t),
      out_specs=(whole,) * n_f,
      scratch_shapes=[pltpu.VMEM((2, shard, kv), jnp.bfloat16)],
    )(at, squares, grad, master, first_moment, second_moment, next_block, *flat(next_rest))
    got = [shift(partial[k], "fsdp", -k) for k in range(1, n_f)]
    projected = functools.reduce(jnp.add, [g.astype(jnp.float32) for g in got], partial[0])
    new_master, new_first, new_second = pl.pallas_call(
      functools.partial(update_kernel, count),
      grid=(2, shard // block),
      out_shape=(shard_type,) * 3,
      in_specs=[whole] + [tile] * 4,
      out_specs=(tile,) * 3,
    )(squares, grad, master, first_moment, second_moment)
    return (new_master, new_first, new_second, projected.astype(jnp.bfloat16))


def solution(mesh):
    in_specs = (
        P(("dp", "fsdp"), None),
        P(("dp", "fsdp"), None),
        P(None, ("dp", "fsdp"), "tensor"),
        P(None, "fsdp", "tensor"),
        P(None, "fsdp", "tensor"),
        P(None, "fsdp", "tensor"),
    )
    out_specs = (
        P(None, "fsdp", "tensor"),
        P(None, "fsdp", "tensor"),
        P(None, "fsdp", "tensor"),
        P(None, ("dp", "fsdp"), "tensor"),
    )
    return jax.shard_map(per_device, mesh=mesh, in_specs=in_specs, out_specs=out_specs, check_vma=False)
```

```python
import functools
from typing import NamedTuple

import jax
import jax.numpy as jnp
from jax import lax
from jax.experimental import pallas as pl
from jax.experimental.pallas import tpu as pltpu
from jax.sharding import PartitionSpec as P

STEP = 10
VMEM = pl.BlockSpec(memory_space=pltpu.VMEM)
HBM = pl.BlockSpec(memory_space=pl.ANY)
SMEM = pl.BlockSpec(memory_space=pltpu.SMEM)
PARAMS = pltpu.CompilerParams(vmem_limit_bytes=12 * 2**20)


class Plan(NamedTuple):
    sources: int
    n_t: int
    outs: tuple


def near(x):
    return pltpu.with_memory_space_constraint(x, pltpu.VMEM)


def far(x):
    return pltpu.with_memory_space_constraint(x, pltpu.HBM)


def shift(x, axis, k):
    n = lax.axis_size(axis)
    return lax.ppermute(x, axis, [(i, (i + k) % n) for i in range(n)])


def trade(x, axis, k):
    n = lax.axis_size(axis)
    return lax.ppermute(x, axis, [(i, i ^ k) for i in range(n)])


def spread(pieces, axis):
    n = lax.axis_size(axis)
    held = {0: list(pieces)}
    stride = n // 2
    while stride:
        for r, group in list(held.items()):
            if stride == 1 and len(group) > 1:
                group = [jnp.concatenate(group, axis=0)]
            moved = []
            for piece in group:
                moved.append(lax.ppermute(piece, axis, [(j, j ^ stride) for j in range(n)]))
            held[r ^ stride] = moved
        stride //= 2
    return [held[r] for r in range(n)]


def contract_rows(a, b):
    return lax.dot_general(a, b, (((0,), (0,)), ((), ())), preferred_element_type=jnp.float32)


def row_blocks(refs, rows):
    return [ref[i : i + rows, :] for ref in refs for i in range(0, ref.shape[0], rows)]


def split(refs, sizes):
    groups = []
    for size in sizes:
        groups.append(refs[:size])
        refs = refs[size:]
    return groups, refs


def grad_kernel(sizes, n_f, own, at_ref, *refs):
    tokens, refs = split(refs, sizes)
    cots, refs = refs[:n_f], refs[n_f:]
    rows, chunk = cots[0].shape[1], tokens[0][0].shape[1]
    squares = jnp.zeros((8, 128), jnp.float32)
    for r, group in enumerate(tokens):
        at = pl.multiple_of((at_ref[0] ^ r) * chunk, chunk)
        for s in range(2):
            blocks = row_blocks(group, rows)
            acc = functools.reduce(jnp.add, [contract_rows(b, c[s]) for b, c in zip(blocks, cots, strict=True)])
            if own:
                refs[0][s, pl.ds(at, chunk), :] = acc
            else:
                acc += refs[0][s, pl.ds(at, chunk), :]
                refs[1][s, pl.ds(at, chunk), :] = acc
                squares += jnp.sum((acc * acc).reshape(-1, 8, 128), axis=0)
    if not own:
        refs[2][...] = squares


def clip_scale(squares, count):
    total = jnp.sum(squares)
    return jnp.minimum(1.0, 1.0 / jnp.sqrt(jnp.full((8, 128), total / count, jnp.float32) + 1e-06))[:1, :1]


def adam_update(scale, grad, master, first_moment, second_moment):
    clipped = scale * grad
    new_first = 0.9 * first_moment + 0.1 * clipped
    new_second = 0.95 * second_moment + (0.05 * clipped) * clipped
    second_hat = new_second * (1.0 / (1.0 - 0.95**STEP))
    root = second_hat * lax.rsqrt(second_hat)
    step = (0.003 / (1.0 - 0.9**STEP)) * new_first / (root + 1e-08)
    new_master = (1.0 - 0.003 * 0.1) * master - step
    return (new_master, new_first, new_second)


def project_kernel(sizes, rows, n_f, count, at_ref, squares_ref, grad_ref, master_ref, m_ref, v_ref, *refs):
    tokens, refs = split(refs, sizes)
    outs, weight = refs[:n_f], refs[n_f]
    chunk, shard = tokens[0][0].shape[1], weight.shape[1]
    block = min(shard, 128)
    scale = clip_scale(squares_ref[...], count)
    for s in range(2):

        def update_block(b, carry, s=s):
            part = pl.ds(pl.multiple_of(b * block, block), block)
            at = (s, part, slice(None))
            new_master, _, _ = adam_update(scale, grad_ref[at], master_ref[at], m_ref[at], v_ref[at])
            weight[at] = new_master.astype(jnp.bfloat16)
            return carry

        lax.fori_loop(0, shard // block, update_block, 0)
        blocks = [row_blocks(group, rows) for group in tokens]
        for k in range(n_f):
            acc = jnp.zeros(outs[0].shape[1:], jnp.float32)
            for r, group in enumerate(blocks):
                at = pl.multiple_of((at_ref[0] ^ r) * chunk, chunk)
                acc += jnp.dot(group[k], weight[s, pl.ds(at, chunk), :], preferred_element_type=jnp.float32)
            outs[k][s] = acc.astype(outs[k].dtype)


def stage_kernel(plan, at_ref, *refs):
    sources, outs, sems = refs[: plan.sources], refs[plan.sources : -1], refs[-1]
    copies = []
    for out, (source, block) in zip(outs, plan.outs, strict=True):
        ref = sources[source]
        if block is not None:
            chunk = out.shape[1]
            owner, r = block
            column = ((at_ref[1] ^ owner) * plan.n_t + (at_ref[0] ^ r)) * chunk
            ref = ref.at[:, pl.ds(pl.multiple_of(column, chunk), chunk)]
        copies.append(pltpu.make_async_copy(ref, out, sems.at[len(copies)]))
        copies[-1].start()
    for copy in copies:
        copy.wait()


def update_kernel(count, squares_ref, grad_ref, master_ref, m_ref, v_ref, *refs):
    outs, held, sems = refs[:3], refs[3:6], refs[6]
    shard = grad_ref.shape[1]
    block = min(shard, 128)
    span = min(shard, 512)
    scale = clip_scale(squares_ref[...], count)
    copies = []
    for s in range(2):
        for first in range(0, shard, span):

            def update_block(b, carry, s=s, first=first):
                at = (s, pl.ds(pl.multiple_of(first + b * block, block), block), slice(None))
                new = adam_update(scale, grad_ref[at], master_ref[at], m_ref[at], v_ref[at])
                for ref, value in zip(held, new, strict=True):
                    ref[at] = value
                return carry

            lax.fori_loop(0, span // block, update_block, 0)
            at = (s, pl.ds(first, span))
            for i in range(3):
                copies.append(pltpu.make_async_copy(held[i].at[at], outs[i].at[at], sems.at[len(copies)]))
                copies[-1].start()
    for copy in copies:
        copy.wait()


def per_device(tokens, next_tokens, cotangent, master, first_moment, second_moment):
    n_f, n_t = lax.axis_size("fsdp"), lax.axis_size("tensor")
    f, t = lax.axis_index("fsdp"), lax.axis_index("tensor")
    rows, width = tokens.shape
    shard = width // n_f
    chunk = shard // n_t
    kv = cotangent.shape[2]
    count = 2.0 * width * kv * n_t
    at = jnp.stack([t, f]).astype(jnp.int32)
    shard_shape = (2, shard, kv)

    def mine(x, owner, r=0):
        return lax.dynamic_slice(x, (0, (f ^ owner) * shard + (t ^ r) * chunk), (rows, chunk))

    def fetch(pieces):
        return [trade(piece, "fsdp", k) for k, piece in enumerate(pieces, 1)]

    state = (master, first_moment, second_moment)
    blocks = [(3, (0, r)) for r in range(n_t)] + [(4, (0, r)) for r in range(n_t)]
    blocks += [(4, (k, 0)) for k in range(1, n_f)]
    by_copy = chunk % 128 == 0
    outs = [(i, None) for i in range(3)] + (blocks if by_copy else [])
    staged = pl.pallas_call(
        functools.partial(stage_kernel, Plan(5, n_t, tuple(outs))),
        out_shape=(pltpu.VMEM(shard_shape, jnp.float32),) * 3
        + (pltpu.VMEM((rows, chunk), jnp.bfloat16),) * (len(outs) - 3),
        in_specs=[SMEM] + [HBM] * 5,
        out_specs=(VMEM,) * len(outs),
        scratch_shapes=[pltpu.SemaphoreType.DMA((len(outs),))],
        compiler_params=pltpu.CompilerParams(vmem_limit_bytes=2**20),
    )(at, *map(far, state), far(tokens), far(next_tokens))
    state, staged = staged[:3], staged[3:]
    if not by_copy:
        staged = [mine((tokens, next_tokens)[source - 3], owner, r) for source, (owner, r) in blocks]
    first, next_first, next_others = staged[:n_t], staged[n_t : 2 * n_t], staged[2 * n_t :]

    rest = fetch([mine(tokens, k) for k in range(1, n_f)])
    other = [shift(x, "dp", 1) for x in [mine(tokens, 0)] + rest]
    other = spread(other, "tensor")
    rest = spread(rest, "tensor")
    cots = [cotangent]
    for k in range(1, n_f):
        bit = k & -k
        cots.append(trade(cots[k ^ bit], "fsdp", bit))
    other_cots = [shift(c, "dp", 1) for c in cots]
    next_rest = spread(fetch(next_others), "tensor")

    def flat(groups):
        return [near(piece) for group in groups for piece in group], [len(group) for group in groups]

    tokens_in, sizes = flat([[a] + b for a, b in zip(first, rest, strict=True)])
    grad = pl.pallas_call(
        functools.partial(grad_kernel, sizes, n_f, True),
        out_shape=pltpu.VMEM(shard_shape, jnp.float32),
        in_specs=[SMEM] + [VMEM] * (len(tokens_in) + n_f),
        out_specs=VMEM,
        compiler_params=PARAMS,
    )(at, *tokens_in, *map(near, cots))
    tokens_in, sizes = flat(other)
    grad, squares = pl.pallas_call(
        functools.partial(grad_kernel, sizes, n_f, False),
        out_shape=(pltpu.VMEM(shard_shape, jnp.float32), jax.ShapeDtypeStruct((8, 128), jnp.float32)),
        in_specs=[SMEM] + [VMEM] * (len(tokens_in) + n_f + 1),
        out_specs=(VMEM, VMEM),
        compiler_params=PARAMS,
    )(at, *tokens_in, *map(near, other_cots), grad)

    for axis, n in (("fsdp", n_f), ("tensor", n_t)):
        squares = functools.reduce(jnp.add, [shift(squares, axis, k) for k in range(1, n)], squares)

    out = (2, rows, kv)
    tokens_in, sizes = flat([[a] + b for a, b in zip(next_first, next_rest, strict=True)])
    partial = pl.pallas_call(
        functools.partial(project_kernel, sizes, rows, n_f, count),
        out_shape=(jax.ShapeDtypeStruct(out, jnp.float32),)
        + (jax.ShapeDtypeStruct(out, jnp.bfloat16),) * (n_f - 1),
        in_specs=[SMEM] + [VMEM] * (5 + len(tokens_in)),
        out_specs=(VMEM,) * n_f,
        scratch_shapes=[pltpu.VMEM((2, shard, kv), jnp.bfloat16)],
        compiler_params=PARAMS,
    )(at, squares, grad, *state, *tokens_in)
    got = [trade(partial[k], "fsdp", k) for k in range(1, n_f)]
    projected = functools.reduce(jnp.add, [g.astype(jnp.float32) for g in got], partial[0])
    copies = 3 * 2 * (shard // min(shard, 512))
    new_master, new_first, new_second = pl.pallas_call(
        functools.partial(update_kernel, count),
        out_shape=(jax.ShapeDtypeStruct(shard_shape, jnp.float32),) * 3,
        in_specs=[VMEM] * 5,
        out_specs=(HBM,) * 3,
        scratch_shapes=[pltpu.VMEM(shard_shape, jnp.float32)] * 3 + [pltpu.SemaphoreType.DMA((copies,))],
        compiler_params=pltpu.CompilerParams(vmem_limit_bytes=16 * 2**20),
    )(squares, grad, *state)
    return (new_master, new_first, new_second, projected.astype(jnp.bfloat16))


def solution(mesh):
    in_specs = (
        P(("dp", "fsdp"), None),
        P(("dp", "fsdp"), None),
        P(None, ("dp", "fsdp"), "tensor"),
        P(None, "fsdp", "tensor"),
        P(None, "fsdp", "tensor"),
        P(None, "fsdp", "tensor"),
    )
    out_specs = (
        P(None, "fsdp", "tensor"),
        P(None, "fsdp", "tensor"),
        P(None, "fsdp", "tensor"),
        P(None, ("dp", "fsdp"), "tensor"),
    )
    return jax.shard_map(per_device, mesh=mesh, in_specs=in_specs, out_specs=out_specs, check_vma=False)
```

```python
import functools
from typing import NamedTuple

import jax
import jax.numpy as jnp
from jax import lax
from jax.experimental import pallas as pl
from jax.experimental.pallas import tpu as pltpu
from jax.sharding import PartitionSpec as P

STEP = 10
VMEM = pl.BlockSpec(memory_space=pltpu.VMEM)
HBM = pl.BlockSpec(memory_space=pl.ANY)
SMEM = pl.BlockSpec(memory_space=pltpu.SMEM)
PARAMS = pltpu.CompilerParams(vmem_limit_bytes=12 * 2**20)


class Plan(NamedTuple):
    sources: int
    n_t: int
    outs: tuple


def near(x):
    return pltpu.with_memory_space_constraint(x, pltpu.VMEM)


def far(x):
    return pltpu.with_memory_space_constraint(x, pltpu.HBM)


def shift(x, axis, k):
    n = lax.axis_size(axis)
    return lax.ppermute(x, axis, [(i, (i + k) % n) for i in range(n)])


def trade(x, axis, k):
    n = lax.axis_size(axis)
    return lax.ppermute(x, axis, [(i, i ^ k) for i in range(n)])


def spread(pieces, axis):
    n = lax.axis_size(axis)
    held = {0: list(pieces)}
    stride = n // 2
    while stride:
        for r, group in list(held.items()):
            if stride == 1 and len(group) > 1:
                group = [jnp.concatenate(group, axis=0)]
            moved = []
            for piece in group:
                moved.append(lax.ppermute(piece, axis, [(j, j ^ stride) for j in range(n)]))
            held[r ^ stride] = moved
        stride //= 2
    return [held[r] for r in range(n)]


def contract_rows(a, b):
    return lax.dot_general(a, b, (((0,), (0,)), ((), ())), preferred_element_type=jnp.float32)


def row_blocks(refs, rows):
    return [ref[i : i + rows, :] for ref in refs for i in range(0, ref.shape[0], rows)]


def split(refs, sizes):
    groups = []
    for size in sizes:
        groups.append(refs[:size])
        refs = refs[size:]
    return groups, refs


def grad_kernel(sizes, n_f, own, at_ref, *refs):
    tokens, refs = split(refs, sizes)
    cots, refs = refs[:n_f], refs[n_f:]
    rows, chunk = cots[0].shape[1], tokens[0][0].shape[1]
    squares = jnp.zeros((8, 128), jnp.float32)
    for r, group in enumerate(tokens):
        at = pl.multiple_of((at_ref[0] ^ r) * chunk, chunk)
        for s in range(2):
            blocks = row_blocks(group, rows)
            acc = functools.reduce(jnp.add, [contract_rows(b, c[s]) for b, c in zip(blocks, cots, strict=True)])
            if own:
                refs[0][s, pl.ds(at, chunk), :] = acc
            else:
                acc += refs[0][s, pl.ds(at, chunk), :]
                refs[1][s, pl.ds(at, chunk), :] = acc
                squares += jnp.sum((acc * acc).reshape(-1, 8, 128), axis=0)
    if not own:
        refs[2][...] = squares


def clip_scale(squares, count):
    total = jnp.sum(squares)
    return jnp.minimum(1.0, 1.0 / jnp.sqrt(jnp.full((8, 128), total / count, jnp.float32) + 1e-06))[:1, :1]


def adam_update(scale, grad, master, first_moment, second_moment):
    clipped = scale * grad
    new_first = 0.9 * first_moment + 0.1 * clipped
    new_second = 0.95 * second_moment + (0.05 * clipped) * clipped
    second_hat = new_second * (1.0 / (1.0 - 0.95**STEP))
    root = second_hat * lax.rsqrt(second_hat)
    step = (0.003 / (1.0 - 0.9**STEP)) * new_first / (root + 1e-08)
    new_master = (1.0 - 0.003 * 0.1) * master - step
    return (new_master, new_first, new_second)


def project_rows(at, tokens, weight, s):
    chunk = tokens[0].shape[1]
    acc = None
    for r, block in enumerate(tokens):
        part = pl.ds(pl.multiple_of((at ^ r) * chunk, chunk), chunk)
        term = jnp.dot(block, weight[s, part, :], preferred_element_type=jnp.float32)
        acc = term if acc is None else acc + term
    return acc


def project_kernel(n_t, count, at_ref, squares_ref, grad_ref, master_ref, m_ref, v_ref, *refs):
    tokens, (weight, out) = refs[:n_t], refs[n_t:]
    shard = weight.shape[1]
    block = min(shard, 128)
    scale = clip_scale(squares_ref[...], count)
    for s in range(2):

        def update_block(b, carry, s=s):
            part = pl.ds(pl.multiple_of(b * block, block), block)
            at = (s, part, slice(None))
            new_master, _, _ = adam_update(scale, grad_ref[at], master_ref[at], m_ref[at], v_ref[at])
            weight[at] = new_master.astype(jnp.bfloat16)
            return carry

        lax.fori_loop(0, shard // block, update_block, 0)
        out[s] = project_rows(at_ref[0], [ref[...] for ref in tokens], weight, s).astype(out.dtype)


def finish_kernel(sizes, rows, at_ref, weight, *refs):
    tokens, outs = split(refs, sizes)
    blocks = [row_blocks(group, rows) for group in tokens]
    for s in range(2):
        for k, out in enumerate(outs):
            out[s] = project_rows(at_ref[0], [group[k] for group in blocks], weight, s).astype(out.dtype)


def stage_kernel(plan, at_ref, *refs):
    sources, outs, sems = refs[: plan.sources], refs[plan.sources : -1], refs[-1]
    copies = []
    for out, (source, block) in zip(outs, plan.outs, strict=True):
        ref = sources[source]
        if block is not None:
            chunk = out.shape[1]
            owner, r = block
            column = ((at_ref[1] ^ owner) * plan.n_t + (at_ref[0] ^ r)) * chunk
            ref = ref.at[:, pl.ds(pl.multiple_of(column, chunk), chunk)]
        copies.append(pltpu.make_async_copy(ref, out, sems.at[len(copies)]))
        copies[-1].start()
    for copy in copies:
        copy.wait()


def update_kernel(count, squares_ref, grad_ref, master_ref, m_ref, v_ref, *refs):
    outs, held, sems = refs[:3], refs[3:6], refs[6]
    shard = grad_ref.shape[1]
    block = min(shard, 128)
    span = min(shard, 512)
    scale = clip_scale(squares_ref[...], count)
    copies = []
    for s in range(2):
        for first in range(0, shard, span):

            def update_block(b, carry, s=s, first=first):
                at = (s, pl.ds(pl.multiple_of(first + b * block, block), block), slice(None))
                new = adam_update(scale, grad_ref[at], master_ref[at], m_ref[at], v_ref[at])
                for ref, value in zip(held, new, strict=True):
                    ref[at] = value
                return carry

            lax.fori_loop(0, span // block, update_block, 0)
            at = (s, pl.ds(first, span))
            for i in range(3):
                copies.append(pltpu.make_async_copy(held[i].at[at], outs[i].at[at], sems.at[len(copies)]))
                copies[-1].start()
    for copy in copies:
        copy.wait()


def per_device(tokens, next_tokens, cotangent, master, first_moment, second_moment):
    n_f, n_t = lax.axis_size("fsdp"), lax.axis_size("tensor")
    f, t = lax.axis_index("fsdp"), lax.axis_index("tensor")
    rows, width = tokens.shape
    shard = width // n_f
    chunk = shard // n_t
    kv = cotangent.shape[2]
    count = 2.0 * width * kv * n_t
    at = jnp.stack([t, f]).astype(jnp.int32)
    shard_shape = (2, shard, kv)

    def mine(x, owner, r=0):
        return lax.dynamic_slice(x, (0, (f ^ owner) * shard + (t ^ r) * chunk), (rows, chunk))

    def fetch(pieces):
        return [trade(piece, "fsdp", k) for k, piece in enumerate(pieces, 1)]

    state = (master, first_moment, second_moment)
    blocks = [(3, (0, r)) for r in range(n_t)] + [(4, (0, r)) for r in range(n_t)]
    blocks += [(4, (k, 0)) for k in range(1, n_f)]
    by_copy = chunk % 128 == 0
    outs = [(i, None) for i in range(3)] + (blocks if by_copy else [])
    staged = pl.pallas_call(
        functools.partial(stage_kernel, Plan(5, n_t, tuple(outs))),
        out_shape=(pltpu.VMEM(shard_shape, jnp.float32),) * 3
        + (pltpu.VMEM((rows, chunk), jnp.bfloat16),) * (len(outs) - 3),
        in_specs=[SMEM] + [HBM] * 5,
        out_specs=(VMEM,) * len(outs),
        scratch_shapes=[pltpu.SemaphoreType.DMA((len(outs),))],
        compiler_params=pltpu.CompilerParams(vmem_limit_bytes=2**20),
    )(at, *map(far, state), far(tokens), far(next_tokens))
    state, staged = staged[:3], staged[3:]
    if not by_copy:
        staged = [mine((tokens, next_tokens)[source - 3], owner, r) for source, (owner, r) in blocks]
    first, next_first, next_others = staged[:n_t], staged[n_t : 2 * n_t], staged[2 * n_t :]

    rest = fetch([mine(tokens, k) for k in range(1, n_f)])
    other = [shift(x, "dp", 1) for x in [mine(tokens, 0)] + rest]
    other = spread(other, "tensor")
    rest = spread(rest, "tensor")
    cots = [cotangent]
    for k in range(1, n_f):
        bit = k & -k
        cots.append(trade(cots[k ^ bit], "fsdp", bit))
    other_cots = [shift(c, "dp", 1) for c in cots]
    next_others = fetch(next_others)
    lead = n_f // 2
    next_lead = spread([next_others.pop(lead - 1)], "tensor")
    next_rest = spread(next_others, "tensor")

    def flat(groups):
        return [near(piece) for group in groups for piece in group], [len(group) for group in groups]

    tokens_in, sizes = flat([[a] + b for a, b in zip(first, rest, strict=True)])
    grad = pl.pallas_call(
        functools.partial(grad_kernel, sizes, n_f, True),
        out_shape=pltpu.VMEM(shard_shape, jnp.float32),
        in_specs=[SMEM] + [VMEM] * (len(tokens_in) + n_f),
        out_specs=VMEM,
        compiler_params=PARAMS,
    )(at, *tokens_in, *map(near, cots))
    tokens_in, sizes = flat(other)
    grad, squares = pl.pallas_call(
        functools.partial(grad_kernel, sizes, n_f, False),
        out_shape=(pltpu.VMEM(shard_shape, jnp.float32), jax.ShapeDtypeStruct((8, 128), jnp.float32)),
        in_specs=[SMEM] + [VMEM] * (len(tokens_in) + n_f + 1),
        out_specs=(VMEM, VMEM),
        compiler_params=PARAMS,
    )(at, *tokens_in, *map(near, other_cots), grad)

    for axis, n in (("tensor", n_t), ("fsdp", n_f)):
        squares = functools.reduce(jnp.add, [shift(squares, axis, k) for k in range(1, n)], squares)

    out = jax.ShapeDtypeStruct((2, rows, kv), jnp.bfloat16)
    tokens_in, _ = flat(next_lead)
    weight, lead_partial = pl.pallas_call(
        functools.partial(project_kernel, n_t, count),
        out_shape=(pltpu.VMEM(shard_shape, jnp.bfloat16), out),
        in_specs=[SMEM] + [VMEM] * (5 + n_t),
        out_specs=(VMEM, VMEM),
        compiler_params=PARAMS,
    )(at, squares, grad, *state, *tokens_in)
    tokens_in, sizes = flat([[a] + b for a, b in zip(next_first, next_rest, strict=True)])
    own, *partial = pl.pallas_call(
        functools.partial(finish_kernel, sizes, rows),
        out_shape=(jax.ShapeDtypeStruct(out.shape, jnp.float32),) + (out,) * (n_f - 2),
        in_specs=[SMEM] + [VMEM] * (1 + len(tokens_in)),
        out_specs=(VMEM,) * (n_f - 1),
        compiler_params=PARAMS,
    )(at, weight, *tokens_in)
    partial.insert(lead - 1, lead_partial)
    got = [trade(x, "fsdp", k) for k, x in enumerate(partial, 1)]
    projected = functools.reduce(jnp.add, [g.astype(jnp.float32) for g in got], own)
    copies = 3 * 2 * (shard // min(shard, 512))
    new_master, new_first, new_second = pl.pallas_call(
        functools.partial(update_kernel, count),
        out_shape=(jax.ShapeDtypeStruct(shard_shape, jnp.float32),) * 3,
        in_specs=[VMEM] * 5,
        out_specs=(HBM,) * 3,
        scratch_shapes=[pltpu.VMEM(shard_shape, jnp.float32)] * 3 + [pltpu.SemaphoreType.DMA((copies,))],
        compiler_params=pltpu.CompilerParams(vmem_limit_bytes=16 * 2**20),
    )(squares, grad, *state)
    return (new_master, new_first, new_second, projected.astype(jnp.bfloat16))


def solution(mesh):
    in_specs = (
        P(("dp", "fsdp"), None),
        P(("dp", "fsdp"), None),
        P(None, ("dp", "fsdp"), "tensor"),
        P(None, "fsdp", "tensor"),
        P(None, "fsdp", "tensor"),
        P(None, "fsdp", "tensor"),
    )
    out_specs = (
        P(None, "fsdp", "tensor"),
        P(None, "fsdp", "tensor"),
        P(None, "fsdp", "tensor"),
        P(None, ("dp", "fsdp"), "tensor"),
    )
    return jax.shard_map(per_device, mesh=mesh, in_specs=in_specs, out_specs=out_specs, check_vma=False)
```
